8 devices in a mesh: col: 2 (over z, y), row: 4 (over x, core).
Axes of the slice: x: 2, y: 2, z: 1, core: 2. Of those that a mesh axis runs over, the one named last changes fastest.
Arguments:
- forcing: float32 [2, 192, 96, 256], P(None, 'row', 'col')
- init_guess: float32 [2, 192, 96, 256], P(None, 'row', 'col')
- cell_coef: float32 [2, 192, 96], P(None, 'row', 'col')
- solve_rows: bfloat16 [2, 4, 2, 2304, 4096], P(None, 'row', 'col')
- relax_factor: float32 [2], replicated
Outputs:
- output: float32 [2, 192, 96, 256], P(None, 'row', 'col')
All inputs are finite; a program needn't handle non-finite values.
Results may differ from the reference program's by a relative error of at most 0.00124.
Values are sent between devices in bfloat16 or wider.
A program may use at most 1 GiB of HBM per device.

```python
import jax
import jax.numpy as jnp
from jax import lax

SUBDOMAIN = 48
MARGIN = 8
RHS_PER_SYS = 256
SWEEPS = 4
BLOCK_ROWS = 4
BLOCK_COLS = 2
SYSTEMS = 2

EXT_SIZE = SUBDOMAIN + 2 * MARGIN
GRID_ROWS = BLOCK_ROWS * SUBDOMAIN
GRID_COLS = BLOCK_COLS * SUBDOMAIN


def face_coefs(coef_grid):
    face_x = jnp.concatenate([coef_grid[:1], 0.5 * (coef_grid[:-1] + coef_grid[1:]), coef_grid[-1:]], axis=0)
    face_y = jnp.concatenate([coef_grid[:, :1], 0.5 * (coef_grid[:, :-1] + coef_grid[:, 1:]), coef_grid[:, -1:]], axis=1)
    return face_x, face_y


def apply_op(face_x, face_y, values):
    wide_x = jnp.pad(values, ((1, 1), (0, 0), (0, 0)))
    wide_y = jnp.pad(values, ((0, 0), (1, 1), (0, 0)))
    flux_x = face_x[:, :, None] * (wide_x[1:] - wide_x[:-1])
    flux_y = face_y[:, :, None] * (wide_y[:, 1:] - wide_y[:, :-1])
    return flux_x[:-1] - flux_x[1:] + flux_y[:, :-1] - flux_y[:, 1:]


def subdomain_inverses(coef_grid):
    face_x, face_y = face_coefs(coef_grid)
    diagonal = face_x[:-1] + face_x[1:] + face_y[:, :-1] + face_y[:, 1:]
    diag_pad = jnp.pad(diagonal, MARGIN, constant_values=1.0)
    couple_x = jnp.pad(face_x[1:-1], MARGIN)
    couple_y = jnp.pad(face_y[:, 1:-1], MARGIN)

    def one_block(block_id):
        row_start = (block_id // BLOCK_COLS) * SUBDOMAIN
        col_start = (block_id % BLOCK_COLS) * SUBDOMAIN
        diag_blk = lax.dynamic_slice(diag_pad, (row_start, col_start), (EXT_SIZE, EXT_SIZE)).reshape(-1)
        link_x = lax.dynamic_slice(couple_x, (row_start, col_start), (EXT_SIZE - 1, EXT_SIZE)).reshape(-1)
        link_y = lax.dynamic_slice(couple_y, (row_start, col_start), (EXT_SIZE, EXT_SIZE - 1))
        link_y = jnp.pad(link_y, ((0, 0), (0, 1))).reshape(-1)[:-1]
        local_op = jnp.diag(diag_blk) - jnp.diag(link_x, EXT_SIZE) - jnp.diag(link_x, -EXT_SIZE) - jnp.diag(link_y, 1) - jnp.diag(link_y, -1)
        full_inv = jnp.linalg.inv(local_op)
        own_rows = full_inv.reshape(EXT_SIZE, EXT_SIZE, EXT_SIZE * EXT_SIZE)[MARGIN:MARGIN + SUBDOMAIN, MARGIN:MARGIN + SUBDOMAIN]
        return own_rows.reshape(SUBDOMAIN * SUBDOMAIN, EXT_SIZE * EXT_SIZE)

    blocks = lax.map(one_block, jnp.arange(BLOCK_ROWS * BLOCK_COLS))
    return blocks.reshape(BLOCK_ROWS, BLOCK_COLS, SUBDOMAIN * SUBDOMAIN, EXT_SIZE * EXT_SIZE)


def setup_inputs(seed: int = 0) -> dict:
    base_key = jax.random.key(seed)
    key_f, key_u, key_c, key_w = jax.random.split(base_key, 4)
    grid_shape = (SYSTEMS, GRID_ROWS, GRID_COLS, RHS_PER_SYS)
    forcing = jax.random.normal(key_f, grid_shape, jnp.float32)
    init_guess = 0.5 * jax.random.normal(key_u, grid_shape, jnp.float32)
    cell_coef = jnp.exp(1.2 * jax.random.uniform(key_c, (SYSTEMS, GRID_ROWS, GRID_COLS), jnp.float32, -1.0, 1.0))
    relax_factor = jax.random.uniform(key_w, (SYSTEMS,), jnp.float32, 0.35, 0.6)
    solve_rows = jnp.stack([subdomain_inverses(cell_coef[system]) for system in range(SYSTEMS)]).astype(jnp.bfloat16)
    return {"forcing": forcing, "init_guess": init_guess, "cell_coef": cell_coef, "solve_rows": solve_rows, "relax_factor": relax_factor}


def solve_system(rhs_grid, start_guess, coef_grid, inv_rows, step_size):
    face_x, face_y = face_coefs(coef_grid)
    flat_rows = inv_rows.reshape(BLOCK_ROWS * BLOCK_COLS, SUBDOMAIN * SUBDOMAIN, EXT_SIZE * EXT_SIZE)
    block_ids = jnp.arange(BLOCK_ROWS * BLOCK_COLS)

    def one_sweep(sweep_state, unused):
        approx, residual = sweep_state
        padded = jnp.pad(residual.astype(jnp.bfloat16), ((MARGIN, MARGIN), (MARGIN, MARGIN), (0, 0)))

        def block_solve(operands):
            block_id, block_mat = operands
            row_start = (block_id // BLOCK_COLS) * SUBDOMAIN
            col_start = (block_id % BLOCK_COLS) * SUBDOMAIN
            window = lax.dynamic_slice(padded, (row_start, col_start, 0), (EXT_SIZE, EXT_SIZE, RHS_PER_SYS))
            return jnp.dot(block_mat, window.reshape(EXT_SIZE * EXT_SIZE, RHS_PER_SYS), preferred_element_type=jnp.float32)

        correction = lax.map(block_solve, (block_ids, flat_rows))
        correction = correction.reshape(BLOCK_ROWS, BLOCK_COLS, SUBDOMAIN, SUBDOMAIN, RHS_PER_SYS).transpose(0, 2, 1, 3, 4).reshape(GRID_ROWS, GRID_COLS, RHS_PER_SYS)
        approx = approx + step_size * correction
        residual = residual - step_size * apply_op(face_x, face_y, correction)
        return (approx, residual), None

    residual = rhs_grid - apply_op(face_x, face_y, start_guess)
    (approx, _), _ = lax.scan(one_sweep, (start_guess, residual), None, length=SWEEPS)
    return approx


def reference(forcing, init_guess, cell_coef, solve_rows, relax_factor):
    results = [solve_system(forcing[system], init_guess[system], cell_coef[system], solve_rows[system], relax_factor[system]) for system in range(SYSTEMS)]
    return jnp.stack(results)
```

```python
import jax
import jax.numpy as jnp
from jax import lax
from jax.experimental import pallas as pl
from jax.experimental.pallas import tpu as pltpu
from jax.sharding import PartitionSpec as P

SWEEPS = 4
SUB = 48
MARGIN = 8
EXT = 64
SYS = 2
RHS = 256
STRIPS = 3
WIDE = 16
LANES = 128
F32 = jnp.float32
BF16 = jnp.bfloat16


def both(face):
    return jnp.concatenate([face, face], axis=1)


def roll_down(values):
    return pltpu.roll(values, 1, 0)


def roll_up(values):
    return pltpu.roll(values, values.shape[0] - 1, 0)


def kernel(f_hbm, u0_hbm, c_ref, s_hbm, om_ref, out_hbm,
           mat, res, apx, cor, win, fx, fy, fyr,
           wys, wxs, wyr, wxr, wcr, zys, zyr, cxr, cyr,
           mat_sem, u_sem, f_sem, out_sem,
           wy_ss, wy_rs, wx_ss, wx_rs, wc_ss, wc_rs,
           zy_ss, zy_rs, zx_ss, zx_rs, cx_ss, cx_rs, cy_ss, cy_rs):
    row = lax.axis_index("row")
    col = lax.axis_index("col")
    has_up = row > 0
    has_dn = row < 3
    left_side = col == 0
    strip_a = 2 * (1 - col)
    strip_c = 2 * col
    tile_off = pl.multiple_of(8 * (1 - col), 8)
    tile_oth = pl.multiple_of(8 * col, 8)
    has_nb = (has_up, has_dn)
    steps = (-1, 1)

    def remote(src, dst, ss, rs, drow, dcol):
        return pltpu.make_async_remote_copy(
            src_ref=src, dst_ref=dst, send_sem=ss, recv_sem=rs,
            device_id={"row": row + drow, "col": col + dcol * (1 - 2 * col)},
            device_id_type=pl.DeviceIdType.MESH)

    def zy_copy(s, par):
        return remote(zys.at[s], zyr.at[par, s], zy_ss.at[s], zy_rs.at[par, s], 0, 1)

    def zx_copy(src, s, d, q):
        start, land = ((1, SUB + 1), (SUB, 0))[d]
        return remote(src.at[s, q, start], src.at[s, q, land], zx_ss.at[s, d, q], zx_rs.at[s, d, q], steps[d], 0)

    def wy_copy(s):
        return remote(wys.at[s], wyr.at[s], wy_ss.at[s], wy_rs.at[s], 0, 1)

    def wx_copy(s, d):
        return remote(wxs.at[s, d], wxr.at[s, d], wx_ss.at[s, d], wx_rs.at[s, d], steps[d], 0)

    def wc_copy(s, d, par):
        first = (0, SUB - MARGIN)[d]
        return remote(wys.at[s, pl.ds(first, MARGIN)], wcr.at[par, s, d], wc_ss.at[par, s, d], wc_rs.at[par, s, d], steps[d], 1)

    def cx_copy(d):
        first = (0, SUB - 8)[d]
        return remote(c_ref.at[:, pl.ds(first, 8), :], cxr.at[d], cx_ss.at[d], cx_rs.at[d], steps[d], 0)

    def cy_copy():
        return remote(c_ref, cyr, cy_ss, cy_rs, 0, 1)

    def start_x(make):
        for d in range(2):
            @pl.when(has_nb[d])
            def _():
                make(d).start()

    def wait_x(make):
        for d in range(2):
            @pl.when(has_nb[d])
            def _():
                make(d).wait_send()

            @pl.when(has_nb[1 - d])
            def _():
                make(d).wait_recv()

    for s in range(SYS):
        for q in range(STRIPS):
            for halo in (0, SUB + 1):
                apx[s, q, halo] = jnp.zeros((WIDE, RHS), F32)
                cor[s, q, halo] = jnp.zeros((WIDE, RHS), F32)

    barrier = pltpu.get_barrier_semaphore()
    for drow in (-1, 0, 1):
        for dcol in (0, 1):
            if drow == 0 and dcol == 0:
                continue

            def greet():
                pl.semaphore_signal(barrier, inc=1, device_id={"row": row + drow, "col": col + dcol * (1 - 2 * col)},
                                    device_id_type=pl.DeviceIdType.MESH)
            if drow == 0:
                greet()
            else:
                pl.when(has_nb[(drow + 1) // 2])(greet)

    def u_load(s, q):
        return pltpu.make_async_copy(u0_hbm.at[s, :, q], apx.at[s, q, pl.ds(1, SUB)], u_sem.at[s, q])

    def f_load(s, q):
        return pltpu.make_async_copy(f_hbm.at[s, :, q], res.at[s, q], f_sem.at[s, q])

    def mat_load(s, q):
        return pltpu.make_async_copy(s_hbm.at[s, :, q], mat.at[s, q], mat_sem.at[s, q])

    for s in range(SYS):
        for q in range(STRIPS):
            u_load(s, q).start()
        for q in range(STRIPS):
            f_load(s, q).start()
    for s in range(SYS):
        for q in (strip_a, 1, strip_c):
            mat_load(s, q).start()

    @pl.loop(0, SYS * EXT * EXT // 256)
    def _(t):
        rows = pl.ds(pl.multiple_of(t * 256, 256), 256)
        win[rows, :] = jnp.zeros((256, RHS), BF16)

    @pl.when(jnp.logical_not(has_up))
    def _():
        for s in range(SYS):
            cxr[1, s, 7:8, :] = c_ref[s, 0:1, :]

    @pl.when(jnp.logical_not(has_dn))
    def _():
        for s in range(SYS):
            cxr[0, s, 0:1, :] = c_ref[s, SUB - 1:SUB, :]

    pl.semaphore_wait(barrier, 1 + 2 * has_up.astype(jnp.int32) + 2 * has_dn.astype(jnp.int32))
    cy_copy().start()
    start_x(cx_copy)

    def send_zy(src, s, par):
        @pl.loop(0, SUB)
        def _(i):
            tile = src[s, strip_a, i + 1, pl.ds(tile_off, 8), :]
            zys[s, i] = jnp.where(left_side, tile[7:8], tile[0:1])
        zy_copy(s, par).start()

    def send_zx(src, s, q):
        start_x(lambda d: zx_copy(src, s, d, q))

    for s in range(SYS):
        for q in range(STRIPS):
            u_load(s, q).wait()
        send_zy(apx, s, 0)
        for q in range(STRIPS):
            send_zx(apx, s, q)

    cy_copy().wait()
    wait_x(cx_copy)
    eye = (lax.broadcasted_iota(jnp.int32, (SUB, SUB), 0) == lax.broadcasted_iota(jnp.int32, (SUB, SUB), 1)).astype(F32)
    lane = lax.broadcasted_iota(jnp.int32, (1, SUB), 1)
    near = (lane == jnp.where(left_side, 0, SUB - 1)).astype(F32)

    def spread(line):
        cells = jnp.sum(jnp.broadcast_to(line, (SUB, SUB)) * eye, axis=1, keepdims=True)
        return jnp.broadcast_to(cells, (SUB, LANES))

    for s in range(SYS):
        def one_row(i, before, s=s):
            line = c_ref[s, pl.ds(i, 1), :]
            here = spread(line)
            face = 0.5 * (before + here)
            other = jnp.broadcast_to(jnp.sum(cyr[s, pl.ds(i, 1), :] * near, axis=1, keepdims=True), (8, LANES))
            first = jnp.broadcast_to(here[0:1], (8, LANES))
            last = jnp.broadcast_to(here[SUB - 1:SUB], (8, LANES))
            beyond = jnp.where(left_side, first, other)
            low = 0.5 * (roll_down(jnp.concatenate([here, beyond], axis=0))[0:SUB] + here)
            high = 0.5 * (last + jnp.where(left_side, other, last))
            for q in range(STRIPS):
                fx[s, q, i] = face[q * WIDE:(q + 1) * WIDE]
                fy[s, q, i] = low[q * WIDE:(q + 1) * WIDE]
            fyr[s, i] = high[0:1]
            return here
        last_row = lax.fori_loop(0, SUB, one_row, spread(cxr[1, s, 7:8, :]))
        face = 0.5 * (last_row + spread(cxr[0, s, 0:1, :]))
        for q in range(STRIPS):
            fx[s, q, SUB] = face[q * WIDE:(q + 1) * WIDE]

    sub = lax.broadcasted_iota(jnp.int32, (8, RHS), 0)
    sub_face = lax.broadcasted_iota(jnp.int32, (8, LANES), 0)

    def frame(src, s, par, scale):
        @pl.loop(0, SUB)
        def _(i):
            near_cols, far_cols = pl.ds(tile_off, 8), pl.ds(tile_oth, 8)
            here = src[s, strip_a, i + 1, near_cols, :]
            inner = src[s, strip_a, i + 1, far_cols, :]
            edge = jnp.broadcast_to(zyr[par, s, i], (8, RHS))
            before = jnp.where(left_side, inner, edge)
            after = jnp.where(left_side, edge, inner)
            lower = jnp.where(sub == 0, roll_down(before), roll_down(here))
            upper = jnp.where(sub == 7, roll_up(after), roll_up(here))
            face = fy[s, strip_a, i, near_cols, :]
            face_after = jnp.where(left_side, jnp.broadcast_to(fyr[s, i], (8, LANES)), fy[s, strip_a, i, far_cols, :])
            face_up = jnp.where(sub_face == 7, roll_up(face_after), roll_up(face))
            applied = both(fx[s, strip_a, i, near_cols, :]) * (here - src[s, strip_a, i, near_cols, :])
            applied += both(fx[s, strip_a, i + 1, near_cols, :]) * (here - src[s, strip_a, i + 2, near_cols, :])
            applied += both(face) * (here - lower)
            applied += both(face_up) * (here - upper)
            wys[s, i] = (res[s, strip_a, i, near_cols, :] - scale * applied).astype(BF16)

    def send_frame(s, par):
        wy_copy(s).start()
        start_x(lambda d: wc_copy(s, d, par))

    def finish(src, s, par, scale, update):
        gap = jnp.zeros((MARGIN, RHS), F32)
        base = s * (EXT * EXT)

        def strips(ref, i):
            return jnp.concatenate([ref[s, q, i] for q in range(STRIPS)], axis=0)

        @pl.loop(0, SUB)
        def _(i):
            here = strips(src, i + 1)
            edge = jnp.broadcast_to(zyr[par, s, i], (8, RHS))
            none = jnp.zeros_like(edge)
            lower = roll_down(jnp.concatenate([here, jnp.where(left_side, none, edge)], axis=0))[0:SUB]
            upper = roll_up(jnp.concatenate([here, jnp.where(left_side, edge, none)], axis=0))[0:SUB]
            face = strips(fy, i)
            face_up = roll_up(jnp.concatenate([face, jnp.broadcast_to(fyr[s, i], (8, LANES))], axis=0))[0:SUB]
            applied = both(strips(fx, i)) * (here - strips(src, i))
            applied += both(strips(fx, i + 1)) * (here - strips(src, i + 2))
            applied += both(face) * (here - lower)
            applied += both(face_up) * (here - upper)
            new = strips(res, i) - scale * applied
            for q in range(STRIPS):
                res[s, q, i] = new[q * WIDE:(q + 1) * WIDE]
            if update:
                for q in range(STRIPS):
                    apx[s, q, i + 1] += scale * src[s, q, i + 1]
            rows = pl.ds(pl.multiple_of(base + (i + MARGIN) * EXT, EXT), EXT)
            win[rows, :] = jnp.concatenate([gap, new, gap], axis=0).astype(BF16)

        @pl.loop(0, MARGIN)
        def _(e):
            wxs[s, 0, e] = strips(res, e).astype(BF16)
            wxs[s, 1, e] = strips(res, e + SUB - MARGIN).astype(BF16)
        start_x(lambda d: wx_copy(s, d))

    def wait_edges(src, s):
        zy_copy(s, 0).wait()
        for q in range(STRIPS):
            wait_x(lambda d: zx_copy(src, s, d, q))

    def fill_halo(s, par):
        base = s * (EXT * EXT)
        wy_copy(s).wait()
        start = pl.multiple_of(SUB * (1 - col), WIDE)

        @pl.loop(0, SUB)
        def _(i):
            rows = pl.ds(pl.multiple_of(base + (i + MARGIN) * EXT + start, WIDE), WIDE)
            old = win[rows, :].astype(F32)
            new = wyr[s, i].astype(F32)
            on_right = jnp.concatenate([old[0:8], new], axis=0)
            on_left = jnp.concatenate([new, old[8:16]], axis=0)
            win[rows, :] = jnp.where(left_side, on_right, on_left).astype(BF16)

        wait_x(lambda d: wx_copy(s, d))
        wait_x(lambda d: wc_copy(s, d, par))
        gap = jnp.zeros((MARGIN, RHS), F32)
        for d in range(2):
            first = (MARGIN + SUB, 0)[d]

            @pl.when(has_nb[1 - d])
            def _():
                @pl.loop(0, MARGIN)
                def _(e):
                    rows = pl.ds(pl.multiple_of(base + (first + e) * EXT, EXT), EXT)
                    corner = wcr[par, s, d, e].astype(F32)
                    parts = [jnp.where(left_side, gap, corner), wxr[s, d, e].astype(F32), jnp.where(left_side, corner, gap)]
                    win[rows, :] = jnp.concatenate(parts, axis=0).astype(BF16)

    def multiply(s, q, first, count):
        window = win[pl.ds(pl.multiple_of(s * (EXT * EXT), EXT * EXT), EXT * EXT), :]
        rows = mat[s, q, first:first + count].reshape(count * WIDE, EXT * EXT)
        out = jnp.dot(rows, window, preferred_element_type=F32)
        cor[s, q, 1 + first:1 + first + count] = out.reshape(count, WIDE, RHS)

    for s in range(SYS):
        for q in range(STRIPS):
            f_load(s, q).wait()
        wait_edges(apx, s)
        frame(apx, s, 0, 1.0)
        send_frame(s, 0)
        finish(apx, s, 0, 1.0, False)

    def out_store(s, q):
        return pltpu.make_async_copy(apx.at[s, q, pl.ds(1, SUB)], out_hbm.at[s, :, q], out_sem.at[s, q])

    def half_sweep(h, carry):
        k = h // 2
        s = h % 2
        par = k % 2
        more = k < SWEEPS - 1
        first_time = k == 0
        scale = om_ref[s]

        def last_strip(q):
            @pl.when(jnp.logical_not(more))
            def _():
                @pl.loop(0, SUB)
                def _(i):
                    apx[s, q, i + 1] += scale * cor[s, q, i + 1]
                out_store(s, q).start()

        def wait_mat(q):
            @pl.when(first_time)
            def _():
                mat_load(s, q).wait()

        fill_halo(s, par)
        wait_mat(strip_a)
        multiply(s, strip_a, 0, SUB)

        @pl.when(more)
        def _():
            send_zy(cor, s, 1 - par)
            send_zx(cor, s, strip_a)
        last_strip(strip_a)

        @pl.when(jnp.logical_and(h > 0, h < 2 * SWEEPS - 1))
        def _():
            s_old = 1 - s
            for q in (1, strip_c):
                wait_x(lambda d: zx_copy(cor, s_old, d, q))
            finish(cor, s_old, ((h - 1) // 2 + 1) % 2, om_ref[s_old], True)

        wait_mat(1)
        multiply(s, 1, 0, SUB)

        @pl.when(more)
        def _():
            send_zx(cor, s, 1)
        last_strip(1)

        wait_mat(strip_c)
        multiply(s, strip_c, 0, SUB // 2)

        @pl.when(more)
        def _():
            zy_copy(s, 1 - par).wait()
            wait_x(lambda d: zx_copy(cor, s, d, strip_a))
            frame(cor, s, 1 - par, scale)
            send_frame(s, 1 - par)

        multiply(s, strip_c, SUB // 2, SUB // 2)

        @pl.when(more)
        def _():
            send_zx(cor, s, strip_c)
        last_strip(strip_c)
        return carry

    lax.fori_loop(0, 2 * SWEEPS, half_sweep, 0)
    for s in range(SYS):
        for q in range(STRIPS):
            out_store(s, q).wait()


def local_solve(forcing, init_guess, cell_coef, solve_rows, relax_factor):
    forcing = forcing.reshape(SYS, SUB, STRIPS, WIDE, RHS)
    init_guess = init_guess.reshape(SYS, SUB, STRIPS, WIDE, RHS)
    mats = solve_rows.reshape(SYS, SUB, STRIPS, WIDE, EXT * EXT)
    hbm = pl.BlockSpec(memory_space=pl.ANY)
    dma = pltpu.SemaphoreType.DMA
    out = pl.pallas_call(
        kernel,
        out_shape=jax.ShapeDtypeStruct((SYS, SUB, STRIPS, WIDE, RHS), F32),
        in_specs=[hbm, hbm, pl.BlockSpec(memory_space=pltpu.VMEM), hbm, pl.BlockSpec(memory_space=pltpu.SMEM)],
        out_specs=hbm,
        scratch_shapes=[
            pltpu.VMEM((SYS, STRIPS, SUB, WIDE, EXT * EXT), BF16),
            pltpu.VMEM((SYS, STRIPS, SUB, WIDE, RHS), F32),
            pltpu.VMEM((SYS, STRIPS, SUB + 2, WIDE, RHS), F32),
            pltpu.VMEM((SYS, STRIPS, SUB + 2, WIDE, RHS), F32),
            pltpu.VMEM((SYS * EXT * EXT, RHS), BF16),
            pltpu.VMEM((SYS, STRIPS, SUB + 1, WIDE, LANES), F32),
            pltpu.VMEM((SYS, STRIPS, SUB, WIDE, LANES), F32),
            pltpu.VMEM((SYS, SUB, 1, LANES), F32),
            pltpu.VMEM((SYS, SUB, MARGIN, RHS), BF16),
            pltpu.VMEM((SYS, 2, MARGIN, SUB, RHS), BF16),
            pltpu.VMEM((SYS, SUB, MARGIN, RHS), BF16),
            pltpu.VMEM((SYS, 2, MARGIN, SUB, RHS), BF16),
            pltpu.VMEM((2, SYS, 2, MARGIN, MARGIN, RHS), BF16),
            pltpu.VMEM((SYS, SUB, 1, RHS), F32),
            pltpu.VMEM((2, SYS, SUB, 1, RHS), F32),
            pltpu.VMEM((2, SYS, 8, SUB), F32),
            pltpu.VMEM((SYS, SUB, SUB), F32),
            dma((SYS, STRIPS)), dma((SYS, STRIPS)), dma((SYS, STRIPS)), dma((SYS, STRIPS)),
            dma((SYS,)), dma((SYS,)), dma((SYS, 2)), dma((SYS, 2)), dma((2, SYS, 2)), dma((2, SYS, 2)),
            dma((SYS,)), dma((2, SYS)), dma((SYS, 2, STRIPS)), dma((SYS, 2, STRIPS)),
            dma((2,)), dma((2,)), dma(()), dma(()),
        ],
        compiler_params=pltpu.CompilerParams(
            collective_id=0, has_side_effects=True, vmem_limit_bytes=67_043_328),
    )(forcing, init_guess, cell_coef, mats, relax_factor)
    return out.reshape(SYS, SUB, SUB, RHS)


def solution(mesh):
    grid_spec = P(None, "row", "col", None)
    return jax.shard_map(
        local_solve, mesh=mesh,
        in_specs=(grid_spec, grid_spec, P(None, "row", "col"), P(None, "row", "col", None, None), P(None)),
        out_specs=grid_spec, check_vma=False)
```

```python
import jax
import jax.numpy as jnp
from jax import lax
from jax.experimental import pallas as pl
from jax.experimental.pallas import tpu as pltpu
from jax.sharding import PartitionSpec as P

SWEEPS = 4
SUB = 48
MARGIN = 8
EXT = 64
SYS = 2
RHS = 256
STRIPS = 3
WIDE = 16
LANES = 128
PIECE = 12
TILES = 16
F32 = jnp.float32
BF16 = jnp.bfloat16


def both(face):
    return jnp.concatenate([face, face], axis=1)


def roll_down(values):
    return pltpu.roll(values, 1, 0)


def roll_up(values):
    return pltpu.roll(values, values.shape[0] - 1, 0)


def kernel(f_hbm, u0_hbm, c_ref, s_hbm, om_ref, out_hbm,
           mat, res, apx, cor0, cor1, win0, win1, fx, fy, fyr,
           wys, wxs, wyr, wxr, wcr, zys, zyr, cxr, cyr,
           mat_sem, u_sem, f_sem, out_sem,
           wy_ss, wy_rs, wx_ss, wx_rs, wc_ss, wc_rs,
           zy_ss, zy_rs, zx_ss, zx_rs, cx_ss, cx_rs, cy_ss, cy_rs):
    row = lax.axis_index("row")
    col = lax.axis_index("col")
    has_up = row > 0
    has_dn = row < 3
    left_side = col == 0
    strip_a = 2 * (1 - col)
    strip_c = 2 * col
    tile_off = pl.multiple_of(8 * (1 - col), 8)
    tile_oth = pl.multiple_of(8 * col, 8)
    has_nb = (has_up, has_dn)
    cors, wins = (cor0, cor1), (win0, win1)
    steps = (-1, 1)

    def remote(src, dst, ss, rs, drow, dcol):
        return pltpu.make_async_remote_copy(
            src_ref=src, dst_ref=dst, send_sem=ss, recv_sem=rs,
            device_id={"row": row + drow, "col": col + dcol * (1 - 2 * col)},
            device_id_type=pl.DeviceIdType.MESH)

    def zy_copy(s, par):
        return remote(zys.at[s], zyr.at[par, s], zy_ss.at[s], zy_rs.at[par, s], 0, 1)

    def zx_copy(s, d, q):
        start, land = ((1, SUB + 1), (SUB, 0))[d]
        return remote(cors[s].at[q, start], cors[s].at[q, land], zx_ss.at[s, d, q], zx_rs.at[s, d, q], steps[d], 0)

    def wy_copy(s, part):
        rows = pl.ds(*((0, MARGIN), (SUB - MARGIN, MARGIN), (MARGIN, SUB - 2 * MARGIN))[part])
        return remote(wys.at[s, rows], wyr.at[s, rows], wy_ss.at[s, part], wy_rs.at[s, part], 0, 1)

    def wx_copy(s, d):
        return remote(wxs.at[s, d], wxr.at[s, d], wx_ss.at[s, d], wx_rs.at[s, d], steps[d], 0)

    def wc_copy(s, d, par):
        first = (0, SUB - MARGIN)[d]
        return remote(wyr.at[s, pl.ds(first, MARGIN)], wcr.at[par, s, d], wc_ss.at[par, s, d], wc_rs.at[par, s, d], steps[d], 0)

    def cx_copy(d):
        first = (0, SUB - 8)[d]
        return remote(c_ref.at[:, pl.ds(first, 8), :], cxr.at[d], cx_ss.at[d], cx_rs.at[d], steps[d], 0)

    def cy_copy():
        return remote(c_ref, cyr, cy_ss, cy_rs, 0, 1)

    def start_x(make):
        for d in range(2):
            @pl.when(has_nb[d])
            def _():
                make(d).start()

    def wait_x(make):
        for d in range(2):
            @pl.when(has_nb[d])
            def _():
                make(d).wait_send()

            @pl.when(has_nb[1 - d])
            def _():
                make(d).wait_recv()

    for s in range(SYS):
        for q in range(STRIPS):
            for halo in (0, SUB + 1):
                cors[s][q, halo] = jnp.zeros((WIDE, RHS), F32)

    barrier = pltpu.get_barrier_semaphore()
    def greet(drow, dcol):
        pl.semaphore_signal(barrier, inc=1, device_id={"row": row + drow, "col": col + dcol * (1 - 2 * col)},
                            device_id_type=pl.DeviceIdType.MESH)

    greet(0, 1)
    for d in range(2):
        @pl.when(has_nb[d])
        def _():
            greet(steps[d], 0)

    def u_load(s, q):
        return pltpu.make_async_copy(u0_hbm.at[s, :, q], cors[s].at[q, pl.ds(1, SUB)], u_sem.at[s, q])

    def f_load(s, q):
        return pltpu.make_async_copy(f_hbm.at[s, :, q], res.at[s, q], f_sem.at[s, q])

    def apx_load(s, q):
        return pltpu.make_async_copy(u0_hbm.at[s, :, q], apx.at[s, q], out_sem.at[s, q])

    def mat_load(s, q, t):
        return pltpu.make_async_copy(s_hbm.at[s, :, q, :, pl.ds(256 * t, 256)], mat.at[s, q, t], mat_sem.at[s, q, t])

    order = (strip_a, 1, strip_c)
    for load in (u_load, f_load):
        for s in range(SYS):
            for q in range(STRIPS):
                load(s, q).start()
    for q in order:
        for t in range(TILES):
            mat_load(0, q, t).start()
    for s in (1, 0):
        for q in range(STRIPS):
            apx_load(s, q).start()
    for q in order:
        for t in range(TILES):
            mat_load(1, q, t).start()

    for s in range(SYS):
        @pl.loop(0, EXT * EXT // 256)
        def _(t):
            rows = pl.ds(pl.multiple_of(t * 256, 256), 256)
            wins[s][rows, :] = jnp.zeros((256, RHS), BF16)

    for d, line, edge in ((1, 7, 0), (0, 0, SUB - 1)):
        @pl.when(jnp.logical_not(has_nb[1 - d]))
        def _():
            for s in range(SYS):
                cxr[d, s, line:line + 1, :] = c_ref[s, edge:edge + 1, :]
                for e in range(MARGIN):
                    wxr[s, d, e] = jnp.zeros((SUB, RHS), BF16)
                    for par in range(2):
                        wcr[par, s, d, e] = jnp.zeros((MARGIN, RHS), BF16)

    pl.semaphore_wait(barrier, 1 + has_up.astype(jnp.int32) + has_dn.astype(jnp.int32))
    cy_copy().start()
    start_x(cx_copy)

    def send_zy(s, par):
        @pl.loop(0, SUB, unroll=8)
        def _(i):
            tile = cors[s][strip_a, i + 1, pl.ds(tile_off, 8), :]
            zys[s, i] = jnp.where(left_side, tile[7:8], tile[0:1])
        zy_copy(s, par).start()

    def send_zx(s, q):
        start_x(lambda d: zx_copy(s, d, q))

    for s in range(SYS):
        for q in range(STRIPS):
            u_load(s, q).wait()
        send_zy(s, 0)
        for q in range(STRIPS):
            send_zx(s, q)

    cy_copy().wait()
    wait_x(cx_copy)
    eye = (lax.broadcasted_iota(jnp.int32, (SUB, SUB), 0) == lax.broadcasted_iota(jnp.int32, (SUB, SUB), 1)).astype(F32)
    lane = lax.broadcasted_iota(jnp.int32, (1, SUB), 1)
    near = (lane == jnp.where(left_side, 0, SUB - 1)).astype(F32)

    def spread(line):
        cells = jnp.sum(jnp.broadcast_to(line, (SUB, SUB)) * eye, axis=1, keepdims=True)
        return jnp.broadcast_to(cells, (SUB, LANES))

    def coefficients(s):
        def one_row(i, before):
            line = c_ref[s, pl.ds(i, 1), :]
            here = spread(line)
            face = 0.5 * (before + here)
            other = jnp.broadcast_to(jnp.sum(cyr[s, pl.ds(i, 1), :] * near, axis=1, keepdims=True), (8, LANES))
            first = jnp.broadcast_to(here[0:1], (8, LANES))
            last = jnp.broadcast_to(here[SUB - 1:SUB], (8, LANES))
            beyond = jnp.where(left_side, first, other)
            low = 0.5 * (roll_down(jnp.concatenate([here, beyond], axis=0))[0:SUB] + here)
            high = 0.5 * (last + jnp.where(left_side, other, last))
            for q in range(STRIPS):
                fx[s, q, i] = face[q * WIDE:(q + 1) * WIDE]
                fy[s, q, i] = low[q * WIDE:(q + 1) * WIDE]
            fyr[s, i] = high[0:1]
            return here
        last_row = lax.fori_loop(0, SUB, one_row, spread(cxr[1, s, 7:8, :]), unroll=4)
        face = 0.5 * (last_row + spread(cxr[0, s, 0:1, :]))
        for q in range(STRIPS):
            fx[s, q, SUB] = face[q * WIDE:(q + 1) * WIDE]

    sub = lax.broadcasted_iota(jnp.int32, (8, RHS), 0)
    sub_face = lax.broadcasted_iota(jnp.int32, (8, LANES), 0)

    def frame_row(s, par, scale, i):
        near_cols, far_cols = pl.ds(tile_off, 8), pl.ds(tile_oth, 8)
        here = cors[s][strip_a, i + 1, near_cols, :]
        inner = cors[s][strip_a, i + 1, far_cols, :]
        edge = jnp.broadcast_to(zyr[par, s, i], (8, RHS))
        before = jnp.where(left_side, inner, edge)
        after = jnp.where(left_side, edge, inner)
        lower = jnp.where(sub == 0, roll_down(before), roll_down(here))
        upper = jnp.where(sub == 7, roll_up(after), roll_up(here))
        face = fy[s, strip_a, i, near_cols, :]
        face_after = jnp.where(left_side, jnp.broadcast_to(fyr[s, i], (8, LANES)), fy[s, strip_a, i, far_cols, :])
        face_up = jnp.where(sub_face == 7, roll_up(face_after), roll_up(face))
        applied = both(fx[s, strip_a, i, near_cols, :]) * (here - cors[s][strip_a, i, near_cols, :])
        applied += both(fx[s, strip_a, i + 1, near_cols, :]) * (here - cors[s][strip_a, i + 2, near_cols, :])
        applied += both(face) * (here - lower)
        applied += both(face_up) * (here - upper)
        wys[s, i] = (res[s, strip_a, i, near_cols, :] - scale * applied).astype(BF16)

    def frame(s, par, scale):
        @pl.loop(0, SUB, unroll=8)
        def _(i):
            frame_row(s, par, scale, i)

    def send_frame(s):
        for part in range(3):
            wy_copy(s, part).start()

    def send_corners(s, par):
        for part in range(2):
            wy_copy(s, part).wait()
        start_x(lambda d: wc_copy(s, d, par))

    def strips(ref, i):
        return jnp.concatenate([ref[q, i] for q in range(STRIPS)], axis=0)

    def finish_row(s, par, scale, gain, i, frame_row=None, below=None):
        gap = jnp.zeros((MARGIN, RHS), F32)
        src = cors[s]
        here = strips(src, i + 1)
        edge = jnp.broadcast_to(zyr[par, s, i], (8, RHS))
        none = jnp.zeros_like(edge)
        before = roll_down(jnp.concatenate([here, jnp.where(left_side, none, edge)], axis=0))
        wide = jnp.concatenate([here, jnp.where(left_side, edge, none)], axis=0)
        face = jnp.concatenate([strips(fy.at[s], i), jnp.broadcast_to(fyr[s, i], (8, LANES))], axis=0)
        flux = both(face) * (wide - before)
        if below is None:
            below = both(strips(fx.at[s], i)) * (here - strips(src, i))
        above = both(strips(fx.at[s], i + 1)) * (strips(src, i + 2) - here)
        applied = (below - above) + (flux[0:SUB] - roll_up(flux)[0:SUB])
        new = strips(res.at[s], i) - scale * applied
        for q in range(STRIPS):
            res[s, q, i] = new[q * WIDE:(q + 1) * WIDE]
            if gain is not None:
                apx[s, q, i] += gain * here[q * WIDE:(q + 1) * WIDE]
        start = (i + MARGIN) * EXT
        rows = pl.ds(start if isinstance(i, int) else pl.multiple_of(start, EXT), EXT)
        wins[s][rows, :] = jnp.concatenate([gap, new, gap], axis=0).astype(BF16)
        if frame_row is not None:
            wxs[(s,) + frame_row] = new.astype(BF16)
        return above

    def finish_rows(s, par, scale, gain, rows, ends):
        held = [None]

        def one(i, first, frame_row):
            held[0] = finish_row(s, par, scale, gain, i, frame_row, None if first else held[0])
        works = []
        for n, i in enumerate(rows):
            frame_row = None if not ends else ((0, i) if i < MARGIN else (1, i - SUB + MARGIN))
            works.append(lambda i=i, first=(n == 0 or rows[n - 1] != i - 1), f=frame_row: one(i, first, f))
        return works

    END_ROWS = list(range(MARGIN)) + list(range(SUB - MARGIN, SUB))

    def send_ends(s):
        start_x(lambda d: wx_copy(s, d))

    def wait_edges(s, which):
        for q in which:
            wait_x(lambda d: zx_copy(s, d, q))

    def fill_tile(s, par, t):
        gap = jnp.zeros((MARGIN, RHS), F32)
        for e in range(4 * t, 4 * t + 4):
            i = e - MARGIN
            if 0 <= i < SUB:
                on_left, on_right = pl.ds(e * EXT, WIDE), pl.ds(e * EXT + SUB, WIDE)
                new = wyr[s, i].astype(F32)
                old = wins[s][on_left, :].astype(F32)
                wins[s][on_left, :] = jnp.concatenate([jnp.where(left_side, gap, new), old[8:16]], axis=0).astype(BF16)
                old = wins[s][on_right, :].astype(F32)
                wins[s][on_right, :] = jnp.concatenate([old[0:8], jnp.where(left_side, new, gap)], axis=0).astype(BF16)
            else:
                d, e_in = (1, e) if i < 0 else (0, i - SUB)
                corner = wcr[par, s, d, e_in].astype(F32)
                parts = [jnp.where(left_side, gap, corner), wxr[s, d, e_in].astype(F32), jnp.where(left_side, corner, gap)]
                wins[s][pl.ds(e * EXT, EXT), :] = jnp.concatenate(parts, axis=0).astype(BF16)

    def product(s, pieces):
        for q, part in pieces:
            rows = pl.ds(PIECE * part, PIECE)
            lhs = jnp.concatenate([mat[s, q, t, rows].reshape(PIECE * WIDE, 256) for t in range(TILES)], axis=1)
            out = jnp.dot(lhs, wins[s][...], preferred_element_type=F32)
            cors[s][q, 1 + PIECE * part:1 + PIECE * part + PIECE] = out.reshape(PIECE, WIDE, RHS)

    coefficients(0)
    for q in range(STRIPS):
        f_load(0, q).wait()
    zy_copy(0, 0).wait()
    wait_edges(0, range(STRIPS))
    frame(0, 0, 1.0)
    send_frame(0)
    for work in finish_rows(0, 0, 1.0, None, END_ROWS, True):
        work()
    send_ends(0)

    @pl.loop(MARGIN, SUB - MARGIN, unroll=2)
    def _(i):
        finish_row(0, 0, 1.0, None, i)

    coefficients(1)
    for q in range(STRIPS):
        f_load(1, q).wait()
    zy_copy(1, 0).wait()
    wait_edges(1, (strip_a,))
    frame(1, 0, 1.0)
    send_frame(1)
    send_corners(0, 0)

    def out_store(s, q):
        return pltpu.make_async_copy(apx.at[s, q], out_hbm.at[s, :, q], out_sem.at[s, q])

    def last_update(q):
        @pl.loop(0, SUB, unroll=4)
        def _(i):
            apx[1, q, i] += om_ref[1] * cors[1][q, i + 1]
        out_store(1, q).start()

    def half_sweep(k, s):
        par = k % 2
        more = k < SWEEPS - 1
        first_time = k == 0
        old = 1 - s
        if s == 0:
            old_par = par
            old_live = k >= 0
            scale = jnp.where(first_time, 1.0, om_ref[old])
            gain = jnp.where(first_time, 0.0, om_ref[old])
        else:
            old_par = 1 - par
            old_live = more
            scale = gain = om_ref[old]

        def wait_mat(q):
            @pl.when(first_time)
            def _():
                for t in range(TILES):
                    mat_load(s, q, t).wait()

        @pl.when(old_live)
        def _():
            wait_edges(old, (1, strip_c))

        @pl.when(first_time)
        def _():
            for q in range(STRIPS):
                apx_load(old, q).wait()
        wait_mat(strip_a)
        wy_copy(s, 2).wait()
        wait_x(lambda d: wx_copy(s, d))
        wait_x(lambda d: wc_copy(s, d, par))

        for t in range(TILES):
            fill_tile(s, par, t)
        product(s, ((strip_a, 0), (strip_a, 2), (strip_a, 1), (strip_a, 3)))
        for work in finish_rows(old, old_par, scale, gain, END_ROWS, True):
            work()

        @pl.when(more)
        def _():
            send_zy(s, 1 - par)
            send_zx(s, strip_a)

        @pl.when(old_live)
        def _():
            send_ends(old)

        wait_mat(1)
        wait_mat(strip_c)
        product(s, ((1, 0), (strip_c, 0), (1, 3), (strip_c, 3)))
        for work in finish_rows(old, old_par, scale, gain, list(range(MARGIN, SUB - MARGIN)), False):
            work()

        @pl.when(more)
        def _():
            send_zx(s, 1)
            send_zx(s, strip_c)

        @pl.when(old_live)
        def _():
            send_corners(old, old_par)
        if s == 1:
            @pl.when(jnp.logical_not(more))
            def _():
                for q in range(STRIPS):
                    out_store(old, q).start()
                last_update(strip_a)

        product(s, ((1, 1), (strip_c, 1)))

        @pl.when(more)
        def _():
            zy_copy(s, 1 - par).wait()
            wait_edges(s, (strip_a,))
            frame(s, 1 - par, om_ref[s])
            send_frame(s)
        product(s, ((1, 2), (strip_c, 2)))

    def sweep(k, carry):
        half_sweep(k, 0)
        half_sweep(k, 1)
        return carry

    lax.fori_loop(0, SWEEPS, sweep, 0)
    last_update(1)
    last_update(strip_c)
    for s in range(SYS):
        for q in range(STRIPS):
            out_store(s, q).wait()


def local_solve(forcing, init_guess, cell_coef, solve_rows, relax_factor):
    forcing = forcing.reshape(SYS, SUB, STRIPS, WIDE, RHS)
    init_guess = init_guess.reshape(SYS, SUB, STRIPS, WIDE, RHS)
    mats = solve_rows.reshape(SYS, SUB, STRIPS, WIDE, EXT * EXT)
    hbm = pl.BlockSpec(memory_space=pl.ANY)
    dma = pltpu.SemaphoreType.DMA
    out = pl.pallas_call(
        kernel,
        out_shape=jax.ShapeDtypeStruct((SYS, SUB, STRIPS, WIDE, RHS), F32),
        in_specs=[hbm, hbm, pl.BlockSpec(memory_space=pltpu.VMEM), hbm, pl.BlockSpec(memory_space=pltpu.SMEM)],
        out_specs=hbm,
        scratch_shapes=[
            pltpu.VMEM((SYS, STRIPS, TILES, SUB, WIDE, 256), BF16),
            pltpu.VMEM((SYS, STRIPS, SUB, WIDE, RHS), F32),
            pltpu.VMEM((SYS, STRIPS, SUB, WIDE, RHS), F32),
            pltpu.VMEM((STRIPS, SUB + 2, WIDE, RHS), F32),
            pltpu.VMEM((STRIPS, SUB + 2, WIDE, RHS), F32),
            pltpu.VMEM((EXT * EXT, RHS), BF16),
            pltpu.VMEM((EXT * EXT, RHS), BF16),
            pltpu.VMEM((SYS, STRIPS, SUB + 1, WIDE, LANES), F32),
            pltpu.VMEM((SYS, STRIPS, SUB, WIDE, LANES), F32),
            pltpu.VMEM((SYS, SUB, 1, LANES), F32),
            pltpu.VMEM((SYS, SUB, MARGIN, RHS), BF16),
            pltpu.VMEM((SYS, 2, MARGIN, SUB, RHS), BF16),
            pltpu.VMEM((SYS, SUB, MARGIN, RHS), BF16),
            pltpu.VMEM((SYS, 2, MARGIN, SUB, RHS), BF16),
            pltpu.VMEM((2, SYS, 2, MARGIN, MARGIN, RHS), BF16),
            pltpu.VMEM((SYS, SUB, 1, RHS), F32),
            pltpu.VMEM((2, SYS, SUB, 1, RHS), F32),
            pltpu.VMEM((2, SYS, 8, SUB), F32),
            pltpu.VMEM((SYS, SUB, SUB), F32),
            dma((SYS, STRIPS, TILES)), dma((SYS, STRIPS)), dma((SYS, STRIPS)), dma((SYS, STRIPS)),
            dma((SYS, 3)), dma((SYS, 3)), dma((SYS, 2)), dma((SYS, 2)), dma((2, SYS, 2)), dma((2, SYS, 2)),
            dma((SYS,)), dma((2, SYS)), dma((SYS, 2, STRIPS)), dma((SYS, 2, STRIPS)),
            dma((2,)), dma((2,)), dma(()), dma(()),
        ],
        compiler_params=pltpu.CompilerParams(
            collective_id=0, has_side_effects=True, vmem_limit_bytes=67_043_328),
    )(forcing, init_guess, cell_coef, mats, relax_factor)
    return out.reshape(SYS, SUB, SUB, RHS)


def solution(mesh):
    grid_spec = P(None, "row", "col", None)
    return jax.shard_map(
        local_solve, mesh=mesh,
        in_specs=(grid_spec, grid_spec, P(None, "row", "col"), P(None, "row", "col", None, None), P(None)),
        out_specs=grid_spec, check_vma=False)
```

```python
import jax
import jax.numpy as jnp
from jax import lax
from jax.experimental import pallas as pl
from jax.experimental.pallas import tpu as pltpu
from jax.sharding import PartitionSpec as P

SWEEPS = 4
SUB = 48
MARGIN = 8
EXT = 64
SYS = 2
RHS = 256
STRIPS = 3
WIDE = 16
LANES = 128
PIECE = 12
EARLY = 20
TILES = 16
F32 = jnp.float32
BF16 = jnp.bfloat16


def both(face):
    return jnp.concatenate([face, face], axis=1)


def roll_down(values):
    return pltpu.roll(values, 1, 0)


def roll_up(values):
    return pltpu.roll(values, values.shape[0] - 1, 0)


def kernel(f_hbm, u0_hbm, c_ref, s_hbm, om_ref, apx,
           mat, res, cor0, cor1, win0, win1, fx, fy, fyr,
           wys, wxs, wyr, wxr, wcr, zys, zyr, cxr, cys, cyr, cyb,
           mat_sem, u_sem, f_sem, out_sem,
           wy_ss, wy_rs, wx_ss, wx_rs, wc_ss, wc_rs,
           zy_ss, zy_rs, zx_ss, zx_rs, cx_ss, cx_rs, cy_ss, cy_rs):
    row = lax.axis_index("row")
    col = lax.axis_index("col")
    has_up = row > 0
    has_dn = row < 3
    left_side = col == 0
    strip_a = 2 * (1 - col)
    strip_c = 2 * col
    tile_off = pl.multiple_of(8 * (1 - col), 8)
    tile_oth = pl.multiple_of(8 * col, 8)
    has_nb = (has_up, has_dn)
    cors, wins = (cor0, cor1), (win0, win1)
    steps = (-1, 1)

    def remote(src, dst, ss, rs, drow, dcol):
        return pltpu.make_async_remote_copy(
            src_ref=src, dst_ref=dst, send_sem=ss, recv_sem=rs,
            device_id={"row": row + drow, "col": col + dcol * (1 - 2 * col)},
            device_id_type=pl.DeviceIdType.MESH)

    def zy_copy(s, par):
        return remote(zys.at[s], zyr.at[par, s], zy_ss.at[s], zy_rs.at[par, s], 0, 1)

    def zx_copy(s, d, part):
        strips_of = (pl.ds(strip_a, 1), pl.ds(col, 2))[part]
        start, land = ((1, SUB + 1), (SUB, 0))[d]
        return remote(cors[s].at[strips_of, start], cors[s].at[strips_of, land],
                      zx_ss.at[s, d, part], zx_rs.at[s, d, part], steps[d], 0)

    def wy_copy(s, part):
        rows = pl.ds(*((0, MARGIN), (SUB - MARGIN, MARGIN), (MARGIN, EARLY), (MARGIN + EARLY, SUB - 2 * MARGIN - EARLY))[part])
        return remote(wys.at[s, rows], wyr.at[s, rows], wy_ss.at[s, part], wy_rs.at[s, part], 0, 1)

    def wx_copy(s, d):
        return remote(wxs.at[s, d], wxr.at[s, d], wx_ss.at[s, d], wx_rs.at[s, d], steps[d], 0)

    def wc_copy(s, d, par):
        first = (0, SUB - MARGIN)[d]
        return remote(wyr.at[s, pl.ds(first, MARGIN)], wcr.at[par, s, d], wc_ss.at[par, s, d], wc_rs.at[par, s, d], steps[d], 0)

    def cx_copy(d):
        first = (0, SUB - 8)[d]
        return remote(c_ref.at[:, pl.ds(first, 8), :], cxr.at[d], cx_ss.at[d], cx_rs.at[d], steps[d], 0)

    def cy_copy():
        return remote(cys, cyr, cy_ss, cy_rs, 0, 1)

    def with_rows(work, cond=None):
        for d in range(2):
            pl.when(has_nb[d] if cond is None else jnp.logical_and(has_nb[d], cond))(lambda d=d: work(d))

    def settle(make, d):
        make(d).wait_send()
        make(1 - d).wait_recv()

    for s in range(SYS):
        for q in range(STRIPS):
            for halo in (0, SUB + 1):
                cors[s][q, halo] = jnp.zeros((WIDE, RHS), F32)

    barrier = pltpu.get_barrier_semaphore()
    def greet(drow, dcol):
        pl.semaphore_signal(barrier, inc=1, device_id={"row": row + drow, "col": col + dcol * (1 - 2 * col)},
                            device_id_type=pl.DeviceIdType.MESH)

    greet(0, 1)
    for d in range(2):
        @pl.when(has_nb[d])
        def _():
            greet(steps[d], 0)

    def u_load(s, q):
        return pltpu.make_async_copy(u0_hbm.at[s, :, q], cors[s].at[q, pl.ds(1, SUB)], u_sem.at[s, q])

    def f_load(s, q):
        return pltpu.make_async_copy(f_hbm.at[s, :, q], res.at[s, q], f_sem.at[s, q])

    def apx_load(s, q):
        return pltpu.make_async_copy(u0_hbm.at[s, :, q], apx.at[s, q], out_sem.at[s, q])

    def mat_load(s, q, t):
        return pltpu.make_async_copy(s_hbm.at[s, :, q, :, pl.ds(256 * t, 256)], mat.at[s, q, t], mat_sem.at[s, q, t])

    order = (strip_a, 1, strip_c)
    for s in range(SYS):
        for load in (u_load, f_load):
            for q in order:
                load(s, q).start()
    for q in order:
        for t in range(TILES):
            mat_load(0, q, t).start()
    for s in (1, 0):
        for q in range(STRIPS):
            apx_load(s, q).start()
    for q in order:
        for t in range(TILES):
            mat_load(1, q, t).start()

    for s in range(SYS):
        @pl.loop(0, EXT * EXT // 256)
        def _(t):
            rows = pl.ds(pl.multiple_of(t * 256, 256), 256)
            wins[s][rows, :] = jnp.zeros((256, RHS), BF16)

    for d, line, edge in ((1, 7, 0), (0, 0, SUB - 1)):
        @pl.when(jnp.logical_not(has_nb[1 - d]))
        def _():
            for s in range(SYS):
                cxr[d, s, line:line + 1, :] = c_ref[s, edge:edge + 1, :]
                for e in range(MARGIN):
                    wxr[s, d, e] = jnp.zeros((SUB, RHS), BF16)
                    for par in range(2):
                        wcr[par, s, d, e] = jnp.zeros((MARGIN, RHS), BF16)

    eye = (lax.broadcasted_iota(jnp.int32, (SUB, SUB), 0) == lax.broadcasted_iota(jnp.int32, (SUB, SUB), 1)).astype(F32)
    lane = lax.broadcasted_iota(jnp.int32, (1, SUB), 1)
    mine = (lane == jnp.where(left_side, SUB - 1, 0)).astype(F32)
    for s in range(SYS):
        column = jnp.sum(c_ref[s] * mine, axis=1, keepdims=True)
        line = jnp.sum(jnp.broadcast_to(column, (SUB, SUB)) * eye, axis=0, keepdims=True)
        cys[s] = jnp.broadcast_to(line, (8, SUB))

    pl.semaphore_wait(barrier, 1 + has_up.astype(jnp.int32) + has_dn.astype(jnp.int32))
    cy_copy().start()
    with_rows(lambda d: cx_copy(d).start())

    def send_zy(s, par):
        @pl.loop(0, SUB, unroll=8)
        def _(i):
            tile = cors[s][strip_a, i + 1, pl.ds(tile_off, 8), :]
            zys[s, i] = jnp.where(left_side, tile[7:8], tile[0:1])
        zy_copy(s, par).start()

    for s in range(SYS):
        u_load(s, strip_a).wait()
        send_zy(s, 0)
        for q in (1, strip_c):
            u_load(s, q).wait()
        with_rows(lambda d: [zx_copy(s, d, part).start() for part in range(2)] and None)

    cy_copy().wait()
    with_rows(lambda d: settle(cx_copy, d))

    def spread(line):
        cells = jnp.sum(jnp.broadcast_to(line, (SUB, SUB)) * eye, axis=1, keepdims=True)
        return jnp.broadcast_to(cells, (SUB, LANES))

    def coefficients(s):
        cyb[...] = spread(cyr[s, 0:1, :])

        def one_row(i, before):
            line = c_ref[s, pl.ds(i, 1), :]
            here = spread(line)
            face = 0.5 * (before + here)
            other = jnp.broadcast_to(cyb[pl.ds(i, 1), :], (8, LANES))
            first = jnp.broadcast_to(here[0:1], (8, LANES))
            last = jnp.broadcast_to(here[SUB - 1:SUB], (8, LANES))
            beyond = jnp.where(left_side, first, other)
            low = 0.5 * (roll_down(jnp.concatenate([here, beyond], axis=0))[0:SUB] + here)
            high = 0.5 * (last + jnp.where(left_side, other, last))
            for q in range(STRIPS):
                fx[s, q, i] = face[q * WIDE:(q + 1) * WIDE]
                fy[s, q, i] = low[q * WIDE:(q + 1) * WIDE]
            fyr[s, i] = high[0:1]
            return here
        last_row = lax.fori_loop(0, SUB, one_row, spread(cxr[1, s, 7:8, :]), unroll=4)
        face = 0.5 * (last_row + spread(cxr[0, s, 0:1, :]))
        for q in range(STRIPS):
            fx[s, q, SUB] = face[q * WIDE:(q + 1) * WIDE]

    sub = lax.broadcasted_iota(jnp.int32, (8, RHS), 0)
    sub_face = lax.broadcasted_iota(jnp.int32, (8, LANES), 0)

    def frame_row(s, par, scale, i):
        near_cols, far_cols = pl.ds(tile_off, 8), pl.ds(tile_oth, 8)
        here = cors[s][strip_a, i + 1, near_cols, :]
        inner = cors[s][strip_a, i + 1, far_cols, :]
        edge = jnp.broadcast_to(zyr[par, s, i], (8, RHS))
        before = jnp.where(left_side, inner, edge)
        after = jnp.where(left_side, edge, inner)
        lower = jnp.where(sub == 0, roll_down(before), roll_down(here))
        upper = jnp.where(sub == 7, roll_up(after), roll_up(here))
        face = fy[s, strip_a, i, near_cols, :]
        face_after = jnp.where(left_side, jnp.broadcast_to(fyr[s, i], (8, LANES)), fy[s, strip_a, i, far_cols, :])
        face_up = jnp.where(sub_face == 7, roll_up(face_after), roll_up(face))
        applied = both(fx[s, strip_a, i, near_cols, :]) * (here - cors[s][strip_a, i, near_cols, :])
        applied += both(fx[s, strip_a, i + 1, near_cols, :]) * (here - cors[s][strip_a, i + 2, near_cols, :])
        applied += both(face) * (here - lower)
        applied += both(face_up) * (here - upper)
        wys[s, i] = (res[s, strip_a, i, near_cols, :] - scale * applied).astype(BF16)

    def frame(s, par, scale):
        @pl.loop(0, SUB, unroll=8)
        def _(i):
            frame_row(s, par, scale, i)

    def send_frame(s):
        for part in range(3):
            wy_copy(s, part).start()

    def send_rest(s):
        wy_copy(s, 3).start()

    def wait_corners(s):
        for part in range(2):
            wy_copy(s, part).wait()

    def strips(ref, i):
        return jnp.concatenate([ref[q, i] for q in range(STRIPS)], axis=0)

    def finish_row(s, par, scale, gain, i, frame_row=None, below=None):
        gap = jnp.zeros((MARGIN, RHS), F32)
        src = cors[s]
        here = strips(src, i + 1)
        edge = jnp.broadcast_to(zyr[par, s, i], (8, RHS))
        none = jnp.zeros_like(edge)
        before = roll_down(jnp.concatenate([here, jnp.where(left_side, none, edge)], axis=0))
        wide = jnp.concatenate([here, jnp.where(left_side, edge, none)], axis=0)
        face = jnp.concatenate([strips(fy.at[s], i), jnp.broadcast_to(fyr[s, i], (8, LANES))], axis=0)
        flux = both(face) * (wide - before)
        if below is None:
            below = both(strips(fx.at[s], i)) * (here - strips(src, i))
        above = both(strips(fx.at[s], i + 1)) * (strips(src, i + 2) - here)
        applied = (below - above) + (flux[0:SUB] - roll_up(flux)[0:SUB])
        new = strips(res.at[s], i) - scale * applied
        for q in range(STRIPS):
            res[s, q, i] = new[q * WIDE:(q + 1) * WIDE]
            if gain is not None:
                apx[s, q, i] += gain * here[q * WIDE:(q + 1) * WIDE]
        start = (i + MARGIN) * EXT
        rows = pl.ds(start if isinstance(i, int) else pl.multiple_of(start, EXT), EXT)
        wins[s][rows, :] = jnp.concatenate([gap, new, gap], axis=0).astype(BF16)
        if frame_row is not None:
            wxs[(s,) + frame_row] = new.astype(BF16)
        return above

    def finish_rows(s, par, scale, gain, rows, ends):
        held = [None]

        def one(i, first, frame_row):
            held[0] = finish_row(s, par, scale, gain, i, frame_row, None if first else held[0])
        works = []
        for n, i in enumerate(rows):
            frame_row = None if not ends else ((0, i) if i < MARGIN else (1, i - SUB + MARGIN))
            works.append(lambda i=i, first=(n == 0 or rows[n - 1] != i - 1), f=frame_row: one(i, first, f))
        return works

    END_ROWS = list(range(MARGIN)) + list(range(SUB - MARGIN, SUB))

    def edges(s, part):
        return lambda d: settle(lambda way: zx_copy(s, way, part), d)

    def fill_tile(s, par, t):
        gap = jnp.zeros((MARGIN, RHS), F32)
        for e in range(4 * t, 4 * t + 4):
            i = e - MARGIN
            if 0 <= i < SUB:
                on_left, on_right = pl.ds(e * EXT, WIDE), pl.ds(e * EXT + SUB, WIDE)
                new = wyr[s, i].astype(F32)
                old = wins[s][on_left, :].astype(F32)
                wins[s][on_left, :] = jnp.concatenate([jnp.where(left_side, gap, new), old[8:16]], axis=0).astype(BF16)
                old = wins[s][on_right, :].astype(F32)
                wins[s][on_right, :] = jnp.concatenate([old[0:8], jnp.where(left_side, new, gap)], axis=0).astype(BF16)
            else:
                d, e_in = (1, e) if i < 0 else (0, i - SUB)
                corner = wcr[par, s, d, e_in].astype(F32)
                parts = [jnp.where(left_side, gap, corner), wxr[s, d, e_in].astype(F32), jnp.where(left_side, corner, gap)]
                wins[s][pl.ds(e * EXT, EXT), :] = jnp.concatenate(parts, axis=0).astype(BF16)

    def product(s, units, works=(), fill=None):
        sums = [None] * len(units)
        done = 0
        for t in range(TILES):
            if fill is not None:
                for ahead in ((0, 1, 2) if t == 0 else (t + 2,)):
                    if ahead < TILES:
                        fill(ahead)
            window = wins[s][256 * t:256 * (t + 1), :]
            for m, pieces in enumerate(units):
                lhs = [mat[s, q, t, pl.ds(PIECE * part, PIECE)].reshape(PIECE * WIDE, 256) for q, part in pieces]
                term = jnp.dot(jnp.concatenate(lhs, axis=0), window, preferred_element_type=F32)
                sums[m] = term if sums[m] is None else sums[m] + term
            upto = len(works) * (t + 1) // (TILES + 1)
            for work in works[done:upto]:
                work()
            done = upto
        for work in works[done:]:
            work()
        for m, pieces in enumerate(units):
            for n, (q, part) in enumerate(pieces):
                rows = slice(PIECE * WIDE * n, PIECE * WIDE * (n + 1))
                cors[s][q, 1 + PIECE * part:1 + PIECE * part + PIECE] = sums[m][rows].reshape(PIECE, WIDE, RHS)

    coefficients(0)
    for q in range(STRIPS):
        f_load(0, q).wait()
    zy_copy(0, 0).wait()
    with_rows(edges(0, 0))
    frame(0, 0, 1.0)
    send_frame(0)
    send_rest(0)
    with_rows(edges(0, 1))
    for work in finish_rows(0, 0, 1.0, None, END_ROWS, True):
        work()
    with_rows(lambda d: wx_copy(0, d).start())

    @pl.loop(MARGIN, SUB - MARGIN, unroll=2)
    def _(i):
        finish_row(0, 0, 1.0, None, i)

    coefficients(1)
    for q in range(STRIPS):
        f_load(1, q).wait()
    zy_copy(1, 0).wait()
    with_rows(edges(1, 0))
    frame(1, 0, 1.0)
    send_frame(1)
    wait_corners(0)
    with_rows(lambda d: wc_copy(0, d, 0).start())

    def last_update(q):
        @pl.loop(0, SUB, unroll=4)
        def _(i):
            apx[1, q, i] += om_ref[1] * cors[1][q, i + 1]

    def half_sweep(k, s):
        par = k % 2
        more = k < SWEEPS - 1
        first_time = k == 0
        old = 1 - s
        if s == 0:
            old_par = par
            old_live = None
            scale = jnp.where(first_time, 1.0, om_ref[old])
            gain = jnp.where(first_time, 0.0, om_ref[old])
        else:
            old_par = 1 - par
            old_live = more
            scale = gain = om_ref[old]

        def when_old(work):
            if old_live is None:
                work()
            else:
                pl.when(old_live)(work)

        def frame_parts(d):
            settle(lambda way: wx_copy(s, way), d)
            settle(lambda way: wc_copy(s, way, par), d)

        @pl.when(first_time)
        def _():
            for q in range(STRIPS):
                apx_load(old, q).wait()
            for t in range(TILES):
                mat_load(s, strip_a, t).wait()
        for part in (2, 3):
            wy_copy(s, part).wait()
        with_rows(frame_parts)

        product(s, (((strip_a, 0), (strip_a, 1)), ((strip_a, 2), (strip_a, 3))),
                finish_rows(old, old_par, scale, gain, END_ROWS[1:-1], True), lambda t: fill_tile(s, par, t))

        @pl.when(more)
        def _():
            send_zy(s, 1 - par)
        with_rows(lambda d: zx_copy(s, d, 0).start(), more)
        when_old(lambda: wy_copy(old, 3).start())
        with_rows(edges(old, 1), old_live)
        for work in finish_rows(old, old_par, scale, gain, END_ROWS[:1] + END_ROWS[-1:], True):
            work()
        with_rows(lambda d: wx_copy(old, d).start(), old_live)

        @pl.when(first_time)
        def _():
            for q in (1, strip_c):
                for t in range(TILES):
                    mat_load(s, q, t).wait()
        product(s, (((1, 0), (strip_c, 0)), ((1, 3), (strip_c, 3))),
                finish_rows(old, old_par, scale, gain, list(range(MARGIN, SUB - MARGIN - 6)), False))
        with_rows(lambda d: zx_copy(s, d, 1).start(), more)
        when_old(lambda: wait_corners(old))
        with_rows(lambda d: wc_copy(old, d, old_par).start(), old_live)

        product(s, (((1, 1),), ((strip_c, 1),)),
                finish_rows(old, old_par, scale, gain, list(range(SUB - MARGIN - 6, SUB - MARGIN)), False))
        if s == 1:
            @pl.when(jnp.logical_not(more))
            def _():
                last_update(strip_a)

        @pl.when(more)
        def _():
            zy_copy(s, 1 - par).wait()
            with_rows(edges(s, 0))
            frame(s, 1 - par, om_ref[s])
            send_frame(s)
        product(s, (((1, 2),), ((strip_c, 2),)))

    def sweep(k, carry):
        half_sweep(k, 0)
        half_sweep(k, 1)
        return carry

    lax.fori_loop(0, SWEEPS, sweep, 0)
    last_update(1)
    last_update(strip_c)


def local_solve(forcing, init_guess, cell_coef, solve_rows, relax_factor):
    forcing = forcing.reshape(SYS, SUB, STRIPS, WIDE, RHS)
    init_guess = init_guess.reshape(SYS, SUB, STRIPS, WIDE, RHS)
    mats = solve_rows.reshape(SYS, SUB, STRIPS, WIDE, EXT * EXT)
    hbm = pl.BlockSpec(memory_space=pl.ANY)
    dma = pltpu.SemaphoreType.DMA
    out = pl.pallas_call(
        kernel,
        out_shape=pltpu.VMEM((SYS, STRIPS, SUB, WIDE, RHS), F32),
        in_specs=[hbm, hbm, pl.BlockSpec(memory_space=pltpu.VMEM), hbm, pl.BlockSpec(memory_space=pltpu.SMEM)],
        out_specs=pl.BlockSpec(memory_space=pltpu.VMEM),
        scratch_shapes=[
            pltpu.VMEM((SYS, STRIPS, TILES, SUB, WIDE, 256), BF16),
            pltpu.VMEM((SYS, STRIPS, SUB, WIDE, RHS), F32),
            pltpu.VMEM((STRIPS, SUB + 2, WIDE, RHS), F32),
            pltpu.VMEM((STRIPS, SUB + 2, WIDE, RHS), F32),
            pltpu.VMEM((EXT * EXT, RHS), BF16),
            pltpu.VMEM((EXT * EXT, RHS), BF16),
            pltpu.VMEM((SYS, STRIPS, SUB + 1, WIDE, LANES), F32),
            pltpu.VMEM((SYS, STRIPS, SUB, WIDE, LANES), F32),
            pltpu.VMEM((SYS, SUB, 1, LANES), F32),
            pltpu.VMEM((SYS, SUB, MARGIN, RHS), BF16),
            pltpu.VMEM((SYS, 2, MARGIN, SUB, RHS), BF16),
            pltpu.VMEM((SYS, SUB, MARGIN, RHS), BF16),
            pltpu.VMEM((SYS, 2, MARGIN, SUB, RHS), BF16),
            pltpu.VMEM((2, SYS, 2, MARGIN, MARGIN, RHS), BF16),
            pltpu.VMEM((SYS, SUB, 1, RHS), F32),
            pltpu.VMEM((2, SYS, SUB, 1, RHS), F32),
            pltpu.VMEM((2, SYS, 8, SUB), F32),
            pltpu.VMEM((SYS, 8, SUB), F32),
            pltpu.VMEM((SYS, 8, SUB), F32),
            pltpu.VMEM((SUB, LANES), F32),
            dma((SYS, STRIPS, TILES)), dma((SYS, STRIPS)), dma((SYS, STRIPS)), dma((SYS, STRIPS)),
            dma((SYS, 4)), dma((SYS, 4)), dma((SYS, 2)), dma((SYS, 2)), dma((2, SYS, 2)), dma((2, SYS, 2)),
            dma((SYS,)), dma((2, SYS)), dma((SYS, 2, 2)), dma((SYS, 2, 2)),
            dma((2,)), dma((2,)), dma(()), dma(()),
        ],
        compiler_params=pltpu.CompilerParams(
            collective_id=0, has_side_effects=True, vmem_limit_bytes=62_000_000),
    )(forcing, init_guess, cell_coef, mats, relax_factor)
    return out.transpose(0, 2, 1, 3, 4).reshape(SYS, SUB, SUB, RHS)


def solution(mesh):
    grid_spec = P(None, "row", "col", None)
    return jax.shard_map(
        local_solve, mesh=mesh,
        in_specs=(grid_spec, grid_spec, P(None, "row", "col"), P(None, "row", "col", None, None), P(None)),
        out_specs=grid_spec, check_vma=False)
```

```python
import jax
import jax.numpy as jnp
from jax import lax
from jax.experimental import pallas as pl
from jax.experimental.pallas import tpu as pltpu
from jax.sharding import PartitionSpec as P

SWEEPS = 4
SUB = 48
MARGIN = 8
EXT = 64
SYS = 2
RHS = 256
STRIPS = 3
WIDE = 16
LANES = 128
PIECE = 12
EARLY = 20
IN_FIRST, IN_SECOND, IN_THIRD = 0, 16, 16
TILES = 16
F32 = jnp.float32
BF16 = jnp.bfloat16


def both(face):
    return jnp.concatenate([face, face], axis=1)


def roll_down(values):
    return pltpu.roll(values, 1, 0)


def roll_up(values):
    return pltpu.roll(values, values.shape[0] - 1, 0)


def kernel(f_hbm, u0_hbm, c_ref, s_hbm, om_ref, apx,
           mat, res, cor0, cor1, win0, win1, fx, fy, fyr,
           wys, wxs, wyr, wxr, wcr, zys, zyr, cxr, cys, cyr, cyb,
           mat_sem, u_sem, f_sem, out_sem,
           wy_ss, wy_rs, wx_ss, wx_rs, wc_ss, wc_rs,
           zy_ss, zy_rs, zx_ss, zx_rs, cx_ss, cx_rs, cy_ss, cy_rs):
    row = lax.axis_index("row")
    col = lax.axis_index("col")
    has_up = row > 0
    has_dn = row < 3
    left_side = col == 0
    strip_a = 2 * (1 - col)
    strip_c = 2 * col
    tile_off = pl.multiple_of(8 * (1 - col), 8)
    tile_oth = pl.multiple_of(8 * col, 8)
    has_nb = (has_up, has_dn)
    cors, wins = (cor0, cor1), (win0, win1)
    steps = (-1, 1)

    def remote(src, dst, ss, rs, drow, dcol):
        return pltpu.make_async_remote_copy(
            src_ref=src, dst_ref=dst, send_sem=ss, recv_sem=rs,
            device_id={"row": row + drow, "col": col + dcol * (1 - 2 * col)},
            device_id_type=pl.DeviceIdType.MESH)

    def zy_copy(s, par):
        return remote(zys.at[s], zyr.at[par, s], zy_ss.at[s], zy_rs.at[par, s], 0, 1)

    def zx_copy(s, d, part):
        strips_of = (pl.ds(strip_a, 1), pl.ds(col, 2))[part]
        start, land = ((1, SUB + 1), (SUB, 0))[d]
        return remote(cors[s].at[strips_of, start], cors[s].at[strips_of, land],
                      zx_ss.at[s, d, part], zx_rs.at[s, d, part], steps[d], 0)

    def wy_copy(s, part):
        rows = pl.ds(*((0, MARGIN), (SUB - MARGIN, MARGIN), (MARGIN, EARLY), (MARGIN + EARLY, SUB - 2 * MARGIN - EARLY))[part])
        return remote(wys.at[s, rows], wyr.at[s, rows], wy_ss.at[s, part], wy_rs.at[s, part], 0, 1)

    def wx_copy(s, d):
        return remote(wxs.at[s, d], wxr.at[s, d], wx_ss.at[s, d], wx_rs.at[s, d], steps[d], 0)

    def wc_copy(s, d, par):
        first = (0, SUB - MARGIN)[d]
        return remote(wyr.at[s, pl.ds(first, MARGIN)], wcr.at[par, s, d], wc_ss.at[par, s, d], wc_rs.at[par, s, d], steps[d], 0)

    def cx_copy(d):
        first = (0, SUB - 8)[d]
        return remote(c_ref.at[:, pl.ds(first, 8), :], cxr.at[d], cx_ss.at[d], cx_rs.at[d], steps[d], 0)

    def cy_copy():
        return remote(cys, cyr, cy_ss, cy_rs, 0, 1)

    def with_rows(work, cond=None):
        for d in range(2):
            pl.when(has_nb[d] if cond is None else jnp.logical_and(has_nb[d], cond))(lambda d=d: work(d))

    def settle(make, d):
        make(d).wait_send()
        make(1 - d).wait_recv()

    for s in range(SYS):
        for q in range(STRIPS):
            for halo in (0, SUB + 1):
                cors[s][q, halo] = jnp.zeros((WIDE, RHS), F32)

    barrier = pltpu.get_barrier_semaphore()
    def greet(drow, dcol):
        pl.semaphore_signal(barrier, inc=1, device_id={"row": row + drow, "col": col + dcol * (1 - 2 * col)},
                            device_id_type=pl.DeviceIdType.MESH)

    greet(0, 1)
    for d in range(2):
        @pl.when(has_nb[d])
        def _():
            greet(steps[d], 0)

    def u_load(s, q):
        return pltpu.make_async_copy(u0_hbm.at[s, :, q], cors[s].at[q, pl.ds(1, SUB)], u_sem.at[s, q])

    def f_load(s, q):
        return pltpu.make_async_copy(f_hbm.at[s, :, q], res.at[s, q], f_sem.at[s, q])

    def apx_load(s, q):
        return pltpu.make_async_copy(u0_hbm.at[s, :, q], apx.at[s, q], out_sem.at[s, q])

    def mat_load(s, q, t):
        return pltpu.make_async_copy(s_hbm.at[s, :, q, :, pl.ds(256 * t, 256)], mat.at[s, q, t], mat_sem.at[s, q, t])

    order = (strip_a, 1, strip_c)
    for s in range(SYS):
        for load in (u_load, f_load):
            for q in order:
                load(s, q).start()
    for q in order:
        for t in range(TILES):
            mat_load(0, q, t).start()
    for s in (1, 0):
        for q in range(STRIPS):
            apx_load(s, q).start()
    for q in order:
        for t in range(TILES):
            mat_load(1, q, t).start()

    for s in range(SYS):
        @pl.loop(0, EXT * EXT // 256)
        def _(t):
            rows = pl.ds(pl.multiple_of(t * 256, 256), 256)
            wins[s][rows, :] = jnp.zeros((256, RHS), BF16)

    for d, line, edge in ((1, 7, 0), (0, 0, SUB - 1)):
        @pl.when(jnp.logical_not(has_nb[1 - d]))
        def _():
            for s in range(SYS):
                cxr[d, s, line:line + 1, :] = c_ref[s, edge:edge + 1, :]
                for e in range(MARGIN):
                    wxr[s, d, e] = jnp.zeros((SUB, RHS), BF16)
                    for par in range(2):
                        wcr[par, s, d, e] = jnp.zeros((MARGIN, RHS), BF16)

    eye = (lax.broadcasted_iota(jnp.int32, (SUB, SUB), 0) == lax.broadcasted_iota(jnp.int32, (SUB, SUB), 1)).astype(F32)
    lane = lax.broadcasted_iota(jnp.int32, (1, SUB), 1)
    mine = (lane == jnp.where(left_side, SUB - 1, 0)).astype(F32)
    for s in range(SYS):
        column = jnp.sum(c_ref[s] * mine, axis=1, keepdims=True)
        line = jnp.sum(jnp.broadcast_to(column, (SUB, SUB)) * eye, axis=0, keepdims=True)
        cys[s] = jnp.broadcast_to(line, (8, SUB))

    pl.semaphore_wait(barrier, 1 + has_up.astype(jnp.int32) + has_dn.astype(jnp.int32))
    cy_copy().start()
    with_rows(lambda d: cx_copy(d).start())

    def send_zy(s, par):
        @pl.loop(0, SUB, unroll=8)
        def _(i):
            tile = cors[s][strip_a, i + 1, pl.ds(tile_off, 8), :]
            zys[s, i] = jnp.where(left_side, tile[7:8], tile[0:1])
        zy_copy(s, par).start()

    for s in range(SYS):
        u_load(s, strip_a).wait()
        send_zy(s, 0)
        for q in (1, strip_c):
            u_load(s, q).wait()
        with_rows(lambda d: [zx_copy(s, d, part).start() for part in range(2)] and None)

    cy_copy().wait()
    with_rows(lambda d: settle(cx_copy, d))

    def spread(line):
        cells = jnp.sum(jnp.broadcast_to(line, (SUB, SUB)) * eye, axis=1, keepdims=True)
        return jnp.broadcast_to(cells, (SUB, LANES))

    def coefficients(s):
        cyb[...] = spread(cyr[s, 0:1, :])

        def one_row(i, before):
            line = c_ref[s, pl.ds(i, 1), :]
            here = spread(line)
            face = 0.5 * (before + here)
            other = jnp.broadcast_to(cyb[pl.ds(i, 1), :], (8, LANES))
            first = jnp.broadcast_to(here[0:1], (8, LANES))
            last = jnp.broadcast_to(here[SUB - 1:SUB], (8, LANES))
            beyond = jnp.where(left_side, first, other)
            low = 0.5 * (roll_down(jnp.concatenate([here, beyond], axis=0))[0:SUB] + here)
            high = 0.5 * (last + jnp.where(left_side, other, last))
            for q in range(STRIPS):
                fx[s, q, i] = face[q * WIDE:(q + 1) * WIDE]
                fy[s, q, i] = low[q * WIDE:(q + 1) * WIDE]
            fyr[s, i] = high[0:1]
            return here
        last_row = lax.fori_loop(0, SUB, one_row, spread(cxr[1, s, 7:8, :]), unroll=4)
        face = 0.5 * (last_row + spread(cxr[0, s, 0:1, :]))
        for q in range(STRIPS):
            fx[s, q, SUB] = face[q * WIDE:(q + 1) * WIDE]

    sub = lax.broadcasted_iota(jnp.int32, (8, RHS), 0)
    sub_face = lax.broadcasted_iota(jnp.int32, (8, LANES), 0)

    def frame_row(s, par, scale, i):
        near_cols, far_cols = pl.ds(tile_off, 8), pl.ds(tile_oth, 8)
        here = cors[s][strip_a, i + 1, near_cols, :]
        inner = cors[s][strip_a, i + 1, far_cols, :]
        edge = jnp.broadcast_to(zyr[par, s, i], (8, RHS))
        before = jnp.where(left_side, inner, edge)
        after = jnp.where(left_side, edge, inner)
        lower = jnp.where(sub == 0, roll_down(before), roll_down(here))
        upper = jnp.where(sub == 7, roll_up(after), roll_up(here))
        face = fy[s, strip_a, i, near_cols, :]
        face_after = jnp.where(left_side, jnp.broadcast_to(fyr[s, i], (8, LANES)), fy[s, strip_a, i, far_cols, :])
        face_up = jnp.where(sub_face == 7, roll_up(face_after), roll_up(face))
        applied = both(fx[s, strip_a, i, near_cols, :]) * (here - cors[s][strip_a, i, near_cols, :])
        applied += both(fx[s, strip_a, i + 1, near_cols, :]) * (here - cors[s][strip_a, i + 2, near_cols, :])
        applied += both(face) * (here - lower)
        applied += both(face_up) * (here - upper)
        wys[s, i] = (res[s, strip_a, i, near_cols, :] - scale * applied).astype(BF16)

    def frame(s, par, scale):
        @pl.loop(0, SUB, unroll=8)
        def _(i):
            frame_row(s, par, scale, i)

    def send_frame(s):
        for part in range(3):
            wy_copy(s, part).start()

    def send_rest(s):
        wy_copy(s, 3).start()

    def wait_corners(s):
        for part in range(2):
            wy_copy(s, part).wait()

    def strips(ref, i):
        return jnp.concatenate([ref[q, i] for q in range(STRIPS)], axis=0)

    def finish_row(s, par, scale, gain, i, frame_row=None, below=None):
        gap = jnp.zeros((MARGIN, RHS), F32)
        src = cors[s]
        here = strips(src, i + 1)
        edge = jnp.broadcast_to(zyr[par, s, i], (8, RHS))
        none = jnp.zeros_like(edge)
        before = roll_down(jnp.concatenate([here, jnp.where(left_side, none, edge)], axis=0))
        wide = jnp.concatenate([here, jnp.where(left_side, edge, none)], axis=0)
        face = jnp.concatenate([strips(fy.at[s], i), jnp.broadcast_to(fyr[s, i], (8, LANES))], axis=0)
        flux = both(face) * (wide - before)
        if below is None:
            below = both(strips(fx.at[s], i)) * (here - strips(src, i))
        above = both(strips(fx.at[s], i + 1)) * (strips(src, i + 2) - here)
        applied = (below - above) + (flux[0:SUB] - roll_up(flux)[0:SUB])
        new = strips(res.at[s], i) - scale * applied
        for q in range(STRIPS):
            res[s, q, i] = new[q * WIDE:(q + 1) * WIDE]
            if gain is not None:
                apx[s, q, i] += gain * here[q * WIDE:(q + 1) * WIDE]
        start = (i + MARGIN) * EXT
        rows = pl.ds(start if isinstance(i, int) else pl.multiple_of(start, EXT), EXT)
        wins[s][rows, :] = jnp.concatenate([gap, new, gap], axis=0).astype(BF16)
        if frame_row is not None:
            wxs[(s,) + frame_row] = new.astype(BF16)
        return above

    def finish_rows(s, par, scale, gain, rows, ends):
        held = [None]

        def one(i, first, frame_row):
            held[0] = finish_row(s, par, scale, gain, i, frame_row, None if first else held[0])
        works = []
        for n, i in enumerate(rows):
            frame_row = None if not ends else ((0, i) if i < MARGIN else (1, i - SUB + MARGIN))
            works.append(lambda i=i, first=(n == 0 or rows[n - 1] != i - 1), f=frame_row: one(i, first, f))
        return works

    END_ROWS = list(range(MARGIN)) + list(range(SUB - MARGIN, SUB))

    def edges(s, part):
        return lambda d: settle(lambda way: zx_copy(s, way, part), d)

    def fill_tile(s, par, t):
        gap = jnp.zeros((MARGIN, RHS), F32)
        for e in range(4 * t, 4 * t + 4):
            i = e - MARGIN
            if 0 <= i < SUB:
                on_left, on_right = pl.ds(e * EXT, WIDE), pl.ds(e * EXT + SUB, WIDE)
                new = wyr[s, i].astype(F32)
                old = wins[s][on_left, :].astype(F32)
                wins[s][on_left, :] = jnp.concatenate([jnp.where(left_side, gap, new), old[8:16]], axis=0).astype(BF16)
                old = wins[s][on_right, :].astype(F32)
                wins[s][on_right, :] = jnp.concatenate([old[0:8], jnp.where(left_side, new, gap)], axis=0).astype(BF16)
            else:
                d, e_in = (1, e) if i < 0 else (0, i - SUB)
                corner = wcr[par, s, d, e_in].astype(F32)
                parts = [jnp.where(left_side, gap, corner), wxr[s, d, e_in].astype(F32), jnp.where(left_side, corner, gap)]
                wins[s][pl.ds(e * EXT, EXT), :] = jnp.concatenate(parts, axis=0).astype(BF16)

    def product(s, units, works=(), order=range(TILES)):
        sums = [None] * len(units)
        done = 0
        for step, t in enumerate(order):
            window = wins[s][256 * t:256 * (t + 1), :]
            for m, pieces in enumerate(units):
                lhs = [mat[s, q, t, pl.ds(PIECE * part, PIECE)].reshape(PIECE * WIDE, 256) for q, part in pieces]
                term = jnp.dot(jnp.concatenate(lhs, axis=0), window, preferred_element_type=F32)
                sums[m] = term if sums[m] is None else sums[m] + term
            upto = len(works) * (step + 1) // (TILES + 1)
            for work in works[done:upto]:
                work()
            done = upto
        for work in works[done:]:
            work()
        for m, pieces in enumerate(units):
            for n, (q, part) in enumerate(pieces):
                rows = slice(PIECE * WIDE * n, PIECE * WIDE * (n + 1))
                cors[s][q, 1 + PIECE * part:1 + PIECE * part + PIECE] = sums[m][rows].reshape(PIECE, WIDE, RHS)

    coefficients(0)
    for q in range(STRIPS):
        f_load(0, q).wait()
    zy_copy(0, 0).wait()
    with_rows(edges(0, 0))
    frame(0, 0, 1.0)
    send_frame(0)
    send_rest(0)
    with_rows(edges(0, 1))
    for work in finish_rows(0, 0, 1.0, None, END_ROWS, True):
        work()
    with_rows(lambda d: wx_copy(0, d).start())

    @pl.loop(MARGIN, SUB - MARGIN, unroll=2)
    def _(i):
        finish_row(0, 0, 1.0, None, i)

    coefficients(1)
    for q in range(STRIPS):
        f_load(1, q).wait()
    zy_copy(1, 0).wait()
    with_rows(edges(1, 0))
    frame(1, 0, 1.0)
    send_frame(1)
    with_rows(edges(1, 1))
    for work in finish_rows(1, 0, 1.0, None, END_ROWS, True):
        work()
    with_rows(lambda d: wx_copy(1, d).start())
    wait_corners(0)
    with_rows(lambda d: wc_copy(0, d, 0).start())

    def last_update(q):
        @pl.loop(0, SUB, unroll=4)
        def _(i):
            apx[1, q, i] += om_ref[1] * cors[1][q, i + 1]

    def half_sweep(k, s):
        par = k % 2
        more = k < SWEEPS - 1
        first_time = k == 0
        old = 1 - s
        if s == 0:
            old_par = par
            old_live = None
            scale = jnp.where(first_time, 1.0, om_ref[old])
            gain = jnp.where(first_time, 0.0, om_ref[old])
        else:
            old_par = 1 - par
            old_live = more
            scale = gain = om_ref[old]

        def when_old(work):
            if old_live is None:
                work()
            else:
                pl.when(old_live)(work)

        def middle(skip, count):
            first = MARGIN + skip
            return finish_rows(old, old_par, scale, gain, list(range(first, first + count)), False)

        def frame_parts(d):
            settle(lambda way: wx_copy(s, way), d)
            settle(lambda way: wc_copy(s, way, par), d)

        @pl.when(first_time)
        def _():
            for q in range(STRIPS if s == 0 else 0):
                apx_load(1, q).wait()
                apx_load(0, q).wait()
            for t in range(TILES):
                mat_load(s, strip_a, t).wait()
        for part in (2, 3):
            wy_copy(s, part).wait()
        for t in range(2, TILES - 2):
            fill_tile(s, par, t)
        with_rows(frame_parts)
        late = (0, 1, TILES - 2, TILES - 1)
        for t in late:
            fill_tile(s, par, t)

        product(s, (((strip_a, 0), (strip_a, 1)), ((strip_a, 2), (strip_a, 3))),
                middle(0, IN_FIRST), tuple(range(2, TILES - 2)) + late)

        @pl.when(more)
        def _():
            send_zy(s, 1 - par)
        with_rows(lambda d: zx_copy(s, d, 0).start(), more)
        when_old(lambda: wy_copy(old, 3).start())

        @pl.when(first_time)
        def _():
            for q in (1, strip_c):
                for t in range(TILES):
                    mat_load(s, q, t).wait()
        product(s, (((1, 0), (strip_c, 0)), ((1, 3), (strip_c, 3))),
                middle(IN_FIRST, IN_SECOND))
        with_rows(lambda d: zx_copy(s, d, 1).start(), more)
        when_old(lambda: wait_corners(old))
        with_rows(lambda d: wc_copy(old, d, old_par).start(), old_live)

        product(s, (((1, 1), (1, 2)), ((strip_c, 1), (strip_c, 2))),
                middle(IN_FIRST + IN_SECOND, IN_THIRD))
        if s == 1:
            @pl.when(jnp.logical_not(more))
            def _():
                last_update(strip_a)

        @pl.when(more)
        def _():
            zy_copy(s, 1 - par).wait()
            with_rows(edges(s, 0))
            frame(s, 1 - par, om_ref[s])
            send_frame(s)
            with_rows(edges(s, 1))
            for work in finish_rows(s, 1 - par, om_ref[s], om_ref[s], END_ROWS, True):
                work()
            with_rows(lambda d: wx_copy(s, d).start())

        if s == 0:
            @pl.when(jnp.logical_not(more))
            def _():
                for q in range(STRIPS):
                    for first in (0, SUB - MARGIN):
                        @pl.loop(first, first + MARGIN, unroll=4)
                        def _(i):
                            apx[0, q, i] += om_ref[0] * cors[0][q, i + 1]

    def sweep(k, carry):
        half_sweep(k, 0)
        half_sweep(k, 1)
        return carry

    lax.fori_loop(0, SWEEPS, sweep, 0)
    last_update(1)
    last_update(strip_c)


def local_solve(forcing, init_guess, cell_coef, solve_rows, relax_factor):
    forcing = forcing.reshape(SYS, SUB, STRIPS, WIDE, RHS)
    init_guess = init_guess.reshape(SYS, SUB, STRIPS, WIDE, RHS)
    mats = solve_rows.reshape(SYS, SUB, STRIPS, WIDE, EXT * EXT)
    hbm = pl.BlockSpec(memory_space=pl.ANY)
    dma = pltpu.SemaphoreType.DMA
    out = pl.pallas_call(
        kernel,
        out_shape=pltpu.VMEM((SYS, STRIPS, SUB, WIDE, RHS), F32),
        in_specs=[hbm, hbm, pl.BlockSpec(memory_space=pltpu.VMEM), hbm, pl.BlockSpec(memory_space=pltpu.SMEM)],
        out_specs=pl.BlockSpec(memory_space=pltpu.VMEM),
        scratch_shapes=[
            pltpu.VMEM((SYS, STRIPS, TILES, SUB, WIDE, 256), BF16),
            pltpu.VMEM((SYS, STRIPS, SUB, WIDE, RHS), F32),
            pltpu.VMEM((STRIPS, SUB + 2, WIDE, RHS), F32),
            pltpu.VMEM((STRIPS, SUB + 2, WIDE, RHS), F32),
            pltpu.VMEM((EXT * EXT, RHS), BF16),
            pltpu.VMEM((EXT * EXT, RHS), BF16),
            pltpu.VMEM((SYS, STRIPS, SUB + 1, WIDE, LANES), F32),
            pltpu.VMEM((SYS, STRIPS, SUB, WIDE, LANES), F32),
            pltpu.VMEM((SYS, SUB, 1, LANES), F32),
            pltpu.VMEM((SYS, SUB, MARGIN, RHS), BF16),
            pltpu.VMEM((SYS, 2, MARGIN, SUB, RHS), BF16),
            pltpu.VMEM((SYS, SUB, MARGIN, RHS), BF16),
            pltpu.VMEM((SYS, 2, MARGIN, SUB, RHS), BF16),
            pltpu.VMEM((2, SYS, 2, MARGIN, MARGIN, RHS), BF16),
            pltpu.VMEM((SYS, SUB, 1, RHS), F32),
            pltpu.VMEM((2, SYS, SUB, 1, RHS), F32),
            pltpu.VMEM((2, SYS, 8, SUB), F32),
            pltpu.VMEM((SYS, 8, SUB), F32),
            pltpu.VMEM((SYS, 8, SUB), F32),
            pltpu.VMEM((SUB, LANES), F32),
            dma((SYS, STRIPS, TILES)), dma((SYS, STRIPS)), dma((SYS, STRIPS)), dma((SYS, STRIPS)),
            dma((SYS, 4)), dma((SYS, 4)), dma((SYS, 2)), dma((SYS, 2)), dma((2, SYS, 2)), dma((2, SYS, 2)),
            dma((SYS,)), dma((2, SYS)), dma((SYS, 2, 2)), dma((SYS, 2, 2)),
            dma((2,)), dma((2,)), dma(()), dma(()),
        ],
        compiler_params=pltpu.CompilerParams(
            collective_id=0, has_side_effects=True, vmem_limit_bytes=62_000_000),
    )(forcing, init_guess, cell_coef, mats, relax_factor)
    return out.transpose(0, 2, 1, 3, 4).reshape(SYS, SUB, SUB, RHS)


def solution(mesh):
    grid_spec = P(None, "row", "col", None)
    return jax.shard_map(
        local_solve, mesh=mesh,
        in_specs=(grid_spec, grid_spec, P(None, "row", "col"), P(None, "row", "col", None, None), P(None)),
        out_specs=grid_spec, check_vma=False)
```
